128 devices in a mesh: groups: 4 (over x, y), section: 32 (over z, core).
Axes of the slice: x: 2, y: 2, z: 16, core: 2. Of those that a mesh axis runs over, the one named last changes fastest.
The devices are a block of a 8x8x16 slice.
Arguments:
- queries: bfloat16 [16384, 4096], P(('groups', 'section')), parts along dimension 0, may hold values from -9 to 9
- slice_keys: bfloat16 [16384, 512], P(('groups', 'section')), parts along dimension 0, may hold values from -6 to 6
- slice_values: bfloat16 [16384, 512], P(('groups', 'section')), parts along dimension 0, may hold values from -6 to 6
- cache_keys: bfloat16 [49152, 512], P(('groups', 'section')), parts along dimension 0, may hold values from -250 to 250
- cache_values: bfloat16 [49152, 512], P(('groups', 'section')), parts along dimension 0, may hold values from -6 to 6
- lent_keys: bfloat16 [128, 3, 1024, 512], P(('groups', 'section')), parts along dimension 0, may hold values from -6 to 6
- lent_values: bfloat16 [128, 3, 1024, 512], P(('groups', 'section')), parts along dimension 0, may hold values from -6 to 6
- lent_len: int32 [128, 3], P(('groups', 'section')), parts along dimension 0, may hold values from 1 to 1024
- slice_index: int32 [128], P(('groups', 'section')), parts along dimension 0, may hold values from 1 to 3
- lend_block: int32 [2, 128, 3], P(None, ('groups', 'section')), parts along dimension 1, may hold values from 0 to 1
- sinks: float32 [64], replicated, may hold values from -1 to 4
- gain: float32 [4096], replicated, may hold values from 0.5 to 2
Outputs:
- first_output: bfloat16 [16384, 4096], P(('groups', 'section')), parts along dimension 0
- second_output: bfloat16 [16384, 4096], P(('groups', 'section')), parts along dimension 0
The draws below stay inside these ranges and needn't reach their ends.
There are 4 independent parts, one for each index of `groups`. The reference program is written for one: setup_inputs(seed, part) draws one part's arguments, and reference() takes and returns one part's arrays. A program takes and returns all parts, laid end to end along the dimension named above; an argument that names none is the same for every part. Nothing has to cross between parts.
All inputs are finite; a program needn't handle non-finite values.
Results may differ from the reference program's by a relative error of at most 0.011.
Values may be sent and summed in bfloat16 or wider, within the bound.
No kernel may reach another device: no remote copies, remote signals or barrier semaphores. Data moves between devices by JAX's collectives and lax.ppermute only.
A program may use at most 128 MiB of HBM per device.

```python
import math
import jax
import jax.numpy as jnp
from jax import lax

QUERY_HEADS = 64
KEY_VALUE_HEADS = 8
HEAD_SIZE = 64
SLICE = 128
QB = 64
CACHE_SLICES = 3
LROWS = 1024
REACH = 3
STEPS = 2
SECTIONS = 32
CACHE = 384
QW = 4096
KVW = 512


def draw_cache_keys(key, part):
    base = jnp.clip(jax.random.normal(key, (SECTIONS, CACHE, KVW), jnp.float32), -6.0, 6.0)
    return base.reshape(SECTIONS * CACHE, KVW).astype(jnp.bfloat16)


def set_ends(result, key, least, top_value):
    longest = result.shape.index(max(result.shape))
    spots = []
    for shift in (0, 1):
        where = [jax.random.randint(jax.random.fold_in(key, axis), (), 0, length) for axis, length in enumerate(result.shape)]
        where[longest] = (where[longest] + shift) % result.shape[longest]
        spots.append(tuple(where))
    return result.at[spots[0]].set(least).at[spots[1]].set(top_value)


def levels(rng, extent, cuts, smallest, largest):
    def one(axis_at, shards_of):
        draws = jax.random.uniform(jax.random.fold_in(jax.random.fold_in(rng, 6), axis_at), (shards_of,), jnp.float32, smallest / len(cuts), largest / len(cuts))
        return jnp.repeat(jnp.exp(draws), extent[axis_at] // shards_of).reshape((-1,) + (1,) * (len(extent) - axis_at - 1))

    level = one(*cuts[0])
    for cut in cuts[1:]:
        level = level * one(*cut)
    return level


def bell_draw(rng, dims, deviation, most, split=(), kind=jnp.bfloat16):
    level = levels(rng, dims, split, -0.22, 0.18) if split else 1.0
    entries = jax.random.normal(rng, dims, jnp.float32) * deviation * level
    return jnp.minimum(jnp.maximum(entries, -most), most).astype(kind)


def setup_inputs(seed: int = 0, part: int = 0) -> dict:
    splits = jax.random.split(jax.random.key(seed), 13)
    part_keys = jax.random.split(jax.random.fold_in(splits[12], part), 13)
    queries = bell_draw(part_keys[0], (SECTIONS * SLICE, QW), 1.5, 9.0, ((0, 32),))
    slice_keys = bell_draw(part_keys[1], (SECTIONS * SLICE, KVW), 1.0, 6.0, ((0, 32),))
    slice_values = bell_draw(part_keys[2], (SECTIONS * SLICE, KVW), 1.0, 6.0, ((0, 32),))
    cache_keys = draw_cache_keys(jax.random.fold_in(jax.random.fold_in(splits[12], part), 71), part)
    cache_values = bell_draw(part_keys[4], (SECTIONS * CACHE, KVW), 1.0, 6.0, ((0, 32),))
    lent_keys = bell_draw(part_keys[5], (SECTIONS, REACH, LROWS, KVW), 1.0, 6.0, ((0, 32),))
    lent_values = bell_draw(part_keys[6], (SECTIONS, REACH, LROWS, KVW), 1.0, 6.0, ((0, 32),))
    lent_len = set_ends(jax.random.randint(part_keys[7], (SECTIONS, REACH), 1, LROWS + 1), jax.random.fold_in(part_keys[7], 1), 1, LROWS).astype(jnp.int32)
    slice_index = set_ends(jax.random.randint(part_keys[8], (SECTIONS,), 1, CACHE_SLICES + 1), jax.random.fold_in(part_keys[8], 1), 1, CACHE_SLICES).astype(jnp.int32)
    lend_block = set_ends(jax.random.randint(part_keys[9], (STEPS, SECTIONS, REACH), 0, SLICE // QB), jax.random.fold_in(part_keys[9], 1), 0, (SLICE // QB) - 1).astype(jnp.int32)
    sinks = jnp.clip(jax.random.uniform(splits[10], (QUERY_HEADS,), jnp.float32, -1.0, 4.0), -1.0, 4.0)
    gain = jnp.clip(jnp.exp(jax.random.uniform(splits[11], (QW,), jnp.float32, math.log(0.5), math.log(2.0))), 0.5, 2.0)
    return {"queries": queries, "slice_keys": slice_keys, "slice_values": slice_values, "cache_keys": cache_keys, "cache_values": cache_values, "lent_keys": lent_keys, "lent_values": lent_values, "lent_len": lent_len, "slice_index": slice_index, "lend_block": lend_block, "sinks": sinks, "gain": gain}


def group_terms(query_matrix, key_rows, value_rows, valid):
    row_count = query_matrix.shape[0]
    group_width = QUERY_HEADS // KEY_VALUE_HEADS
    query_heads = query_matrix.reshape(row_count, KEY_VALUE_HEADS, group_width, HEAD_SIZE).astype(jnp.float32)
    key_heads = key_rows.reshape(-1, KEY_VALUE_HEADS, HEAD_SIZE).astype(jnp.float32)
    value_heads = value_rows.reshape(-1, KEY_VALUE_HEADS, HEAD_SIZE).astype(jnp.float32)
    score = jnp.einsum('rhgd,khd->hgrk', query_heads, key_heads, precision=lax.Precision.HIGHEST) * HEAD_SIZE ** (-0.5)
    score = jnp.where(valid[None, None], score, -jnp.inf)
    peak = lax.optimization_barrier(jnp.max(score, axis=-1))
    weight = jnp.exp(score - peak[..., None])
    total = lax.optimization_barrier(jnp.sum(weight, axis=-1))
    rounded = lax.optimization_barrier(weight.astype(jnp.bfloat16)).astype(jnp.float32)
    summed = jnp.einsum('hgrk,khd->hgrd', rounded, value_heads, precision=lax.Precision.HIGHEST)
    return (peak, total, summed)

def widen(terms, start, row_count):
    peak, total, summed = terms
    full_peak = jnp.full(peak.shape[:2] + (row_count,), -jnp.inf, jnp.float32)
    full_total = jnp.zeros(peak.shape[:2] + (row_count,), jnp.float32)
    full_summed = jnp.zeros(peak.shape[:2] + (row_count, summed.shape[3]), jnp.float32)
    full_peak = lax.dynamic_update_slice_in_dim(full_peak, peak, start, 2)
    full_total = lax.dynamic_update_slice_in_dim(full_total, total, start, 2)
    full_summed = lax.dynamic_update_slice_in_dim(full_summed, summed, start, 2)
    return (full_peak, full_total, full_summed)

def combine(parts, sinks, row_count):
    peaks = jnp.stack([part[0] for part in parts])
    totals = jnp.stack([part[1] for part in parts])
    summeds = jnp.stack([part[2] for part in parts])
    sink_logit = sinks.reshape(KEY_VALUE_HEADS, QUERY_HEADS // KEY_VALUE_HEADS)[:, :, None]
    top = jnp.maximum(lax.optimization_barrier(jnp.max(peaks, axis=0)), sink_logit)
    factor = jnp.exp(peaks - top)
    denom = lax.optimization_barrier(jnp.sum(totals * factor, axis=0)) + jnp.exp(sink_logit - top)
    out = lax.optimization_barrier(jnp.sum(summeds * factor[..., None], axis=0)) / denom[..., None]
    return out.transpose(2, 0, 1, 3).reshape(row_count, QUERY_HEADS * HEAD_SIZE)

def attend(query_all, key_all, value_all, cache_k, cache_v, lent_keys, lent_values, lent_len, slice_index, plan, sinks):
    position = jnp.arange(SLICE, dtype=jnp.int32)
    slice_valid = position[None, :] <= position[:, None]
    cache_pos = jnp.arange(CACHE, dtype=jnp.int32)
    lent_pos = jnp.arange(LROWS, dtype=jnp.int32)

    def one_section(section_id):
        current = query_all[section_id]
        key_rows = jnp.concatenate([cache_k[section_id], key_all[section_id]], axis=0)
        value_rows = jnp.concatenate([cache_v[section_id], value_all[section_id]], axis=0)
        own_rows = slice_index[section_id] * SLICE
        cache_valid = jnp.broadcast_to(cache_pos[None, :] < own_rows, (SLICE, CACHE))
        valid = jnp.concatenate([cache_valid, slice_valid], axis=1)
        parts = [group_terms(current, key_rows, value_rows, valid)]
        for dist in range(REACH):
            target = ((section_id + dist + 1) % SECTIONS).astype(jnp.int32)
            start = (plan[section_id, dist] * QB).astype(jnp.int32)
            block = lax.dynamic_slice_in_dim(current, start, QB, 0)
            lent_valid = jnp.broadcast_to(lent_pos[None, :] < lent_len[target, dist], (QB, LROWS))
            terms = group_terms(block, lent_keys[target, dist], lent_values[target, dist], lent_valid)
            parts.append(widen(terms, start, SLICE))
        return combine(parts, sinks, SLICE)
    return lax.map(one_section, jnp.arange(SECTIONS, dtype=jnp.int32))

def reference(queries, slice_keys, slice_values, cache_keys, cache_values, lent_keys, lent_values, lent_len, slice_index, lend_block, sinks, gain):
    query_all = queries.reshape(SECTIONS, SLICE, QW)
    key_all = slice_keys.reshape(SECTIONS, SLICE, KVW)
    value_all = slice_values.reshape(SECTIONS, SLICE, KVW)
    cache_k = cache_keys.reshape(SECTIONS, CACHE, KVW)
    cache_v = cache_values.reshape(SECTIONS, CACHE, KVW)
    first = attend(query_all, key_all, value_all, cache_k, cache_v, lent_keys, lent_values, lent_len, slice_index, lend_block[0], sinks).astype(jnp.bfloat16)
    stream = query_all.astype(jnp.float32) + first.astype(jnp.float32)
    heads = stream.reshape(SECTIONS, SLICE, QUERY_HEADS, HEAD_SIZE)
    norm = jnp.sqrt(lax.optimization_barrier(jnp.mean(heads * heads, axis=-1, keepdims=True)) + 1e-06)
    next_queries = ((heads / norm).reshape(SECTIONS, SLICE, QW) * gain).astype(jnp.bfloat16)
    moved_q = jnp.roll(next_queries, 1, axis=0)
    moved_k = jnp.roll(key_all, 1, axis=0)
    moved_v = jnp.roll(value_all, 1, axis=0)
    second = attend(moved_q, moved_k, moved_v, cache_k, cache_v, lent_keys, lent_values, lent_len, slice_index, lend_block[1], sinks).astype(jnp.bfloat16)
    return (first.reshape(SECTIONS * SLICE, QW), second.reshape(SECTIONS * SLICE, QW))
```

```python
import math

import jax
import jax.numpy as jnp
from jax import lax
from jax.experimental import pallas as pl
from jax.experimental.pallas import tpu as pltpu
from jax.sharding import PartitionSpec as P

HEAD = 64
GROUP = 8
QB = 64
REACH = 3
LANES = 128
PAIR = 2 * GROUP * HEAD
KEY_BLOCK = 256
TILE = 512
ATTEND_VMEM = 32 << 20
COMBINE_VMEM = 16 << 20
CHUNKS = 2
LOG2E = math.log2(math.e)
SCALE2 = LOG2E * HEAD ** -0.5


def from_behind(block, distance, axis="section"):
    size = lax.axis_size(axis)
    route = [((i - distance) % size, i) for i in range(size)]
    return lax.ppermute(block, axis, route)


def stack_heads(q, parity):
    rows = q.shape[0]
    upper = lax.broadcasted_iota(jnp.int32, (rows, LANES), 1) >= HEAD
    keep = upper if parity else jnp.logical_not(upper)
    stacked = []
    for tile in range(GROUP // 2):
        at = parity * GROUP * HEAD + tile * LANES
        both = q[:, at : at + LANES].astype(jnp.float32)
        turned = pltpu.roll(both, HEAD, 1)
        for half in range(2):
            head = both if half == parity else turned
            stacked.append(jnp.where(keep, head, 0.0).astype(jnp.bfloat16))
    return jnp.concatenate(stacked, axis=0)


def attend_pair(q, keys, values, mask_of, out_ref, lane_at, head_at, stats_at, scores, weights):
    rows, used = q.shape[0], keys.shape[0]
    lane = lax.broadcasted_iota(jnp.int32, (rows, LANES), 1)
    peaks = jnp.zeros((rows, LANES), jnp.float32)
    totals = jnp.ones((rows, LANES), jnp.float32)
    with_ones = jnp.concatenate([values, jnp.ones_like(values)], axis=1)
    for parity in range(2):
        stacked = stack_heads(q, parity)
        for start in range(0, used, KEY_BLOCK):
            score = lax.dot_general(
                stacked,
                keys[start : start + KEY_BLOCK],
                (((1,), (1,)), ((), ())),
                preferred_element_type=jnp.float32,
            )
            scores[parity, :, start : start + KEY_BLOCK] = mask_of(score, start)
    for parity in range(2):
        for head in range(GROUP):
            at = head * rows
            peak = jnp.max(scores[parity, at : at + rows, :used], axis=1, keepdims=True)
            peaks = jnp.where(lane == head_at + parity * GROUP + head, peak, peaks)
            for start in range(0, used, KEY_BLOCK):
                score = scores[parity, at : at + rows, start : start + KEY_BLOCK]
                weights[parity, at : at + rows, start : start + KEY_BLOCK] = jnp.exp2(
                    (score - peak) * SCALE2
                ).astype(jnp.bfloat16)
    for parity in range(2):
        both = jnp.dot(
            weights[parity, :, :used], with_ones, preferred_element_type=jnp.float32
        )
        for tile in range(GROUP // 2):
            halves = []
            for half in range(2):
                head = 2 * tile + half
                part = both[head * rows : (head + 1) * rows]
                total = part[:, LANES:]
                part = part[:, :LANES] / total
                halves.append(part if half == parity else pltpu.roll(part, HEAD, 1))
                totals = jnp.where(lane == head_at + parity * GROUP + head, total, totals)
            joined = jnp.where(lane < HEAD, halves[0], halves[1]).astype(jnp.bfloat16)
            start = pl.multiple_of(lane_at + parity * GROUP * HEAD + tile * LANES, LANES)
            out_ref[:, pl.ds(start, LANES)] = joined
    level = peaks * SCALE2 + jnp.log2(totals)
    high = level.astype(jnp.bfloat16).astype(jnp.float32)
    where = pl.ds(pl.multiple_of(stats_at, LANES), LANES)
    stats = out_ref[:, where].astype(jnp.float32)
    stats = stats + high + pltpu.roll(level - high, HEAD, 1)
    out_ref[:, where] = stats.astype(jnp.bfloat16)


def places(pair, pairs, chunk_pairs):
    chunk, inner = lax.div(pair, chunk_pairs), lax.rem(pair, chunk_pairs)
    return pair * PAIR, inner * 2 * GROUP, pairs * PAIR + chunk * LANES


def clear_stats(pair, out_ref, pairs):
    @pl.when(pair == 0)
    def _():
        width = pairs * PAIR
        out_ref[:, width:] = jnp.zeros(
            (out_ref.shape[0], out_ref.shape[1] - width), jnp.bfloat16
        )


def lent_job(length, q, k_ref, v_ref, out_ref, spots, scores, weights):
    lent_rows = k_ref.shape[2]
    half = lent_rows // 2
    for used, now in ((half, length <= half), (lent_rows, length > half)):

        @pl.when(now)
        def _(used=used):
            def mask_of(score, start):
                if used == lent_rows and start < half:
                    return score
                col = lax.broadcasted_iota(jnp.int32, score.shape, 1)
                return jnp.where(col < length - start, score, -jnp.inf)

            attend_pair(
                q,
                k_ref[0, 0, :used, :],
                v_ref[0, 0, :used, :],
                mask_of,
                out_ref,
                *spots,
                scores,
                weights,
            )


def local_job(count, q, ck_ref, cv_ref, sk_ref, sv_ref, out_ref, spots, scores, weights):
    rows, cache_rows = q.shape[0], ck_ref.shape[0]

    def mask_of(score, start):
        row = lax.rem(lax.broadcasted_iota(jnp.int32, score.shape, 0), rows)
        col = lax.broadcasted_iota(jnp.int32, score.shape, 1) + start
        limit = jnp.where(col < cache_rows, count * rows, row + cache_rows + 1)
        return jnp.where(col < limit, score, -jnp.inf)

    attend_pair(
        q,
        jnp.concatenate([ck_ref[...], sk_ref[...]], axis=0),
        jnp.concatenate([cv_ref[...], sv_ref[...]], axis=0),
        mask_of,
        out_ref,
        *spots,
        scores,
        weights,
    )


def local_kernel(index_ref, q_ref, ck, cv, sk, sv, out_ref, scores, weights, *, pairs, chunk_pairs):
    pair = pl.program_id(0)
    clear_stats(pair, out_ref, pairs)
    spots = places(pair, pairs, chunk_pairs)
    local_job(index_ref[0], q_ref[...], ck, cv, sk, sv, out_ref, spots, scores, weights)


def near_kernel(
    len_ref, plan_ref, q_ref, k_ref, v_ref, out_ref, scores, weights, *, pairs, chunk_pairs
):
    pair = pl.program_id(0)
    clear_stats(pair, out_ref, pairs)
    start = pl.multiple_of(plan_ref[0] * QB, QB)
    q = q_ref[pl.ds(start, QB), :]
    spots = places(pair, pairs, chunk_pairs)
    lent_job(len_ref[0], q, k_ref, v_ref, out_ref, spots, scores, weights)


def home_kernel(
    index_ref, len_ref, plan_ref, q_ref, ck, cv, sk, sv, k_ref, v_ref,
    own_ref, near_ref, scores, weights, near_scores, near_weights, *, pairs, chunk_pairs
):
    local_kernel(
        index_ref, q_ref, ck, cv, sk, sv, own_ref, scores, weights,
        pairs=pairs, chunk_pairs=chunk_pairs,
    )
    near_kernel(
        len_ref, plan_ref, q_ref, k_ref, v_ref, near_ref, near_scores, near_weights,
        pairs=pairs, chunk_pairs=chunk_pairs,
    )


def away_kernel(len_ref, *refs, pairs):
    reach = REACH - 1
    q_refs, (k_ref, v_ref) = refs[:reach], refs[reach : reach + 2]
    out_refs, (scores, weights, out) = refs[reach + 2 : 2 * reach + 2], refs[2 * reach + 2 :]
    dist, pair = pl.program_id(0), pl.program_id(1)
    clear_stats(pair, out, pairs)
    q = jnp.where(dist == 0, q_refs[0][...], q_refs[1][...])
    lent_job(
        len_ref[dist + 1], q, k_ref, v_ref, out, places(pair, pairs, pairs), scores, weights
    )
    for d in range(reach):

        @pl.when(jnp.logical_and(dist == d, pair == pairs - 1))
        def _(d=d):
            out_refs[d][...] = out[...]


def scratch(rows, keys):
    return [
        pltpu.VMEM((2, GROUP * rows, keys), jnp.float32),
        pltpu.VMEM((2, GROUP * rows, keys), jnp.bfloat16),
    ]


def estimate(rows, heads, keys):
    return pl.CostEstimate(
        flops=16 * rows * heads * keys * HEAD, bytes_accessed=4 << 20, transcendentals=0
    )


def specs_of(q, cache_keys, near_keys, chunk, pairs):
    rows, base = q.shape[0], chunk * pairs
    q_base = base if q.shape[1] > pairs * PAIR else 0
    q_spec = pl.BlockSpec((rows, PAIR), lambda i, *_: (0, q_base + i))
    cache_spec = pl.BlockSpec((cache_keys.shape[0], LANES), lambda i, *_: (0, base + i))
    own_spec = pl.BlockSpec((rows, LANES), lambda i, *_: (0, base + i))
    near_spec = pl.BlockSpec(
        (1, 1, near_keys.shape[2], LANES), lambda i, *_: (0, 0, 0, base + i)
    )
    return q_spec, [cache_spec, cache_spec, own_spec, own_spec], [near_spec, near_spec]


def packed(rows, pairs, chunk_pairs):
    width = pairs * PAIR + pairs // chunk_pairs * LANES
    return (
        jax.ShapeDtypeStruct((rows, width), jnp.bfloat16),
        pl.BlockSpec((rows, width), lambda i, *_: (0, 0)),
    )


def home_calls(parts, scalars, q, own, near, chunk, pairs, chunk_pairs):
    index, lengths, plan = scalars
    rows = q.shape[0]
    q_spec, own_specs, near_specs = specs_of(q, own[0], near[0], chunk, pairs)
    own_out, own_out_spec = packed(rows, pairs, chunk_pairs)
    near_out, near_out_spec = packed(QB, pairs, chunk_pairs)
    keys = own[0].shape[0] + own[2].shape[0]
    lent_rows = near[0].shape[2]
    kernel, ins, specs, outs, out_specs, buffers, cost = {
        "local": (
            local_kernel, (index, q, *own), own_specs, own_out, own_out_spec,
            scratch(rows, keys), estimate(rows, 16 * pairs, keys),
        ),
        "near": (
            near_kernel, (lengths, plan, q, *near), near_specs, near_out, near_out_spec,
            scratch(QB, lent_rows), estimate(QB, 16 * pairs, lent_rows),
        ),
        "home": (
            home_kernel, (index, lengths, plan, q, *own, *near), own_specs + near_specs,
            [own_out, near_out], [own_out_spec, near_out_spec],
            scratch(rows, keys) + scratch(QB, lent_rows),
            estimate(rows, 32 * pairs, keys),
        ),
    }[parts]
    return pl.pallas_call(
        lambda *refs: kernel(*refs, pairs=pairs, chunk_pairs=chunk_pairs),
        grid_spec=pltpu.PrefetchScalarGridSpec(
            num_scalar_prefetch=len(ins) - len(specs) - 1,
            grid=(pairs,),
            in_specs=[q_spec] + specs,
            out_specs=out_specs,
            scratch_shapes=buffers,
        ),
        out_shape=outs,
        cost_estimate=cost,
        compiler_params=pltpu.CompilerParams(vmem_limit_bytes=ATTEND_VMEM),
        name=parts,
    )(*ins)


def away_call(lengths, blocks, keys, values, chunk, pairs):
    reach = REACH - 1
    lent_rows = keys.shape[2]
    width = pairs * PAIR + LANES
    kv_spec = pl.BlockSpec(
        (1, 1, lent_rows, LANES), lambda d, i, *_: (0, d + 1, 0, chunk * pairs + i)
    )
    return pl.pallas_call(
        lambda *refs: away_kernel(*refs, pairs=pairs),
        grid_spec=pltpu.PrefetchScalarGridSpec(
            num_scalar_prefetch=1,
            grid=(reach, pairs),
            in_specs=[
                pl.BlockSpec((QB, PAIR), lambda d, i, *_: (0, jnp.where(d == 0, i, pairs - 1))),
                pl.BlockSpec((QB, PAIR), lambda d, i, *_: (0, jnp.where(d == 0, 0, i))),
                kv_spec,
                kv_spec,
            ],
            out_specs=[pl.BlockSpec((QB, width), lambda d, i, *_: (0, 0))] * reach,
            scratch_shapes=scratch(QB, lent_rows) + [pltpu.VMEM((QB, width), jnp.bfloat16)],
        ),
        out_shape=[jax.ShapeDtypeStruct((QB, width), jnp.bfloat16)] * reach,
        cost_estimate=estimate(QB, 32 * pairs, lent_rows),
        compiler_params=pltpu.CompilerParams(vmem_limit_bytes=ATTEND_VMEM),
        name="away",
    )(lengths, *blocks, keys, values)


def two_parts(x):
    high = x.astype(jnp.bfloat16)
    low = (x - high.astype(jnp.float32)).astype(jnp.bfloat16)
    return jnp.concatenate([high, low], axis=1)


def picks(count, first, parts=2):
    shape = (parts * count, TILE)
    head = lax.div(lax.broadcasted_iota(jnp.int32, shape, 1), HEAD) + first
    row = lax.rem(lax.broadcasted_iota(jnp.int32, shape, 0), count)
    return jnp.where(head == row, 1.0, 0.0).astype(jnp.bfloat16)


def combine_kernel(plan_ref, *refs, heads, form_next, aliased):
    groups = REACH + 1
    data, stats = refs[:groups], refs[groups : 2 * groups]
    sink_ref, rest = refs[2 * groups], refs[2 * groups + 1 :]
    if form_next:
        q_ref, gain_ref = rest[:2]
        rest = rest[2:]
    rest = rest[aliased:]
    out_ref = rest[0]
    acc, levels, parts = rest[-3:]
    rows = data[0].shape[0]
    step = pl.program_id(0)
    starts = [pl.multiple_of(plan_ref[d] * QB, QB) for d in range(REACH)]

    @pl.when(step == 0)
    def _():
        def level_of(ref):
            both = ref[...].astype(jnp.float32)
            return both[:, :heads] + both[:, HEAD : HEAD + heads]

        sink = sink_ref[...] * LOG2E
        levels[1:] = jnp.full((REACH, rows, heads), -jnp.inf, jnp.float32)
        levels[0] = level_of(stats[0])
        for d in range(REACH):
            levels[d + 1, pl.ds(starts[d], QB), :] = level_of(stats[d + 1])
        top = jnp.maximum(levels[0], sink)
        for d in range(REACH):
            top = jnp.maximum(top, levels[d + 1])
        denom = jnp.exp2(sink - top)
        for g in range(groups):
            weight = jnp.exp2(levels[g] - top)
            denom = denom + weight
            levels[g] = weight
        share = 1.0 / denom
        parts[:rows, :] = two_parts(levels[0] * share)
        levels[0] = share
        for d in range(REACH):
            at = pl.ds(starts[d], QB)
            parts[rows + d * QB : rows + (d + 1) * QB, :] = two_parts(
                levels[d + 1, at, :] * levels[0, at, :]
            )

    spread = jnp.dot(
        parts[...], picks(heads, step * (TILE // HEAD)), preferred_element_type=jnp.float32
    )
    acc[...] = data[0][...].astype(jnp.float32) * spread[:rows]
    for d in range(REACH):
        at = pl.ds(starts[d], QB)
        share = spread[rows + d * QB : rows + (d + 1) * QB]
        acc[at, :] = acc[at, :] + data[d + 1][...].astype(jnp.float32) * share
    out = acc[...].astype(jnp.bfloat16)
    out_ref[...] = out
    if form_next:
        stream = q_ref[...].astype(jnp.float32) + out.astype(jnp.float32)
        count = LANES // 2
        pick = picks(count, 0)
        high_low = two_parts(stream * stream)
        pick_sum = picks(LANES, 0, 1)
        contract = (((1,), (1,)), ((), ()))
        sums = lax.dot_general(
            high_low[:, :TILE], pick_sum, contract, preferred_element_type=jnp.float32
        ) + lax.dot_general(
            high_low[:, TILE:], pick_sum, contract, preferred_element_type=jnp.float32
        )
        inverse = lax.rsqrt(sums[:, :count] * (1.0 / HEAD) + 1e-06)
        factor = jnp.dot(two_parts(inverse), pick, preferred_element_type=jnp.float32)
        rest[1][...] = (stream * factor * gain_ref[...]).astype(jnp.bfloat16)


def combine_call(plan, groups, sinks, before, chunk, chunk_heads, queries=None, gain=None):
    rows = groups[0].shape[0]
    width = chunk_heads * HEAD
    tiles = width // TILE
    whole_width = CHUNKS * width
    form_next = queries is not None
    data_specs, stats_specs = [], []
    for group in groups:
        wide = group.shape[1] > width + LANES
        base = chunk * tiles if wide else 0
        stat = whole_width // LANES + chunk if wide else width // LANES
        data_specs.append(
            pl.BlockSpec((group.shape[0], TILE), lambda i, *_, base=base: (0, base + i))
        )
        stats_specs.append(
            pl.BlockSpec((group.shape[0], LANES), lambda i, *_, stat=stat: (0, stat))
        )
    ins = [plan, *groups, *groups, sinks]
    specs = data_specs + stats_specs + [pl.BlockSpec((1, chunk_heads), lambda i, *_: (0, 0))]
    place = pl.BlockSpec((rows, TILE), lambda i, *_: (0, chunk * tiles + i))
    outs = [jax.ShapeDtypeStruct((rows, whole_width), jnp.bfloat16)]
    out_specs = [place]
    if form_next:
        ins += [queries, gain]
        specs += [place, pl.BlockSpec((1, TILE), lambda i, *_: (0, chunk * tiles + i))]
        outs.append(jax.ShapeDtypeStruct((rows, width), jnp.bfloat16))
        out_specs.append(pl.BlockSpec((rows, TILE), lambda i, *_: (0, i)))
    aliases = {}
    if before is not None:
        aliases = {len(ins): 0}
        ins.append(before)
        specs.append(pl.BlockSpec(memory_space=pl.ANY))
    return pl.pallas_call(
        lambda *refs: combine_kernel(
            *refs, heads=chunk_heads, form_next=form_next, aliased=len(aliases)
        ),
        grid_spec=pltpu.PrefetchScalarGridSpec(
            num_scalar_prefetch=1,
            grid=(tiles,),
            in_specs=specs,
            out_specs=out_specs,
            scratch_shapes=[
                pltpu.VMEM((rows, TILE), jnp.float32),
                pltpu.VMEM((REACH + 1, rows, chunk_heads), jnp.float32),
                pltpu.VMEM((rows + REACH * QB, 2 * chunk_heads), jnp.bfloat16),
            ],
        ),
        out_shape=outs,
        input_output_aliases=aliases,
        cost_estimate=pl.CostEstimate(
            flops=1 << 29, bytes_accessed=4 << 20, transcendentals=0
        ),
        compiler_params=pltpu.CompilerParams(vmem_limit_bytes=COMBINE_VMEM),
        name="combine",
    )(*ins)


def body(
    queries,
    slice_keys,
    slice_values,
    cache_keys,
    cache_values,
    lent_keys,
    lent_values,
    lent_len,
    slice_index,
    lend_block,
    sinks,
    gain,
):
    heads = queries.shape[1] // HEAD
    chunk_heads = heads // CHUNKS
    width = chunk_heads * HEAD
    all_pairs = heads // (2 * GROUP)
    pairs = all_pairs // CHUNKS
    plan = lend_block[:, 0, :]
    lengths = lent_len[0]
    gain_row = gain[None, :]
    sink_rows = [sinks[c * chunk_heads : (c + 1) * chunk_heads][None, :] for c in range(CHUNKS)]

    def blocks_of(current, step, lane):
        return [
            lax.dynamic_slice(current, (plan[step, d] * QB, jnp.int32(lane)), (QB, width))
            for d in range(1, REACH)
        ]

    def sent(blocks):
        return [from_behind(block, d + 2) for d, block in enumerate(blocks)]

    def returned(parts):
        return [from_behind(part, -(d + 2)) for d, part in enumerate(parts)]

    def away(arrived, chunk):
        parts = away_call(lengths, arrived, lent_keys, lent_values, chunk, pairs)
        return returned(parts)

    blocks = [blocks_of(queries, 0, c * width) for c in range(CHUNKS)]
    arrived = [sent(block) for block in blocks]
    _, late_keys, late_values = lax.optimization_barrier((blocks, lent_keys, lent_values))
    near = (from_behind(late_keys[:, :1], -1), from_behind(late_values[:, :1], -1))
    near_lengths = from_behind(lengths, -1)
    moved_own = (
        cache_keys,
        cache_values,
        from_behind(slice_keys, 1),
        from_behind(slice_values, 1),
    )
    own = (cache_keys, cache_values, slice_keys, slice_values)
    scalars = [(slice_index, near_lengths, plan[step]) for step in range(2)]
    local = home_calls("local", scalars[0], queries, own, near, 0, all_pairs, pairs)
    far = [away(arrived[c], c) for c in range(CHUNKS)]
    close = home_calls("near", scalars[0], queries, own, near, 0, all_pairs, pairs)
    first, moved = None, []
    for c in range(CHUNKS):
        first, following = combine_call(
            plan[0], [local, close, *far[c]], sink_rows[c], first, c, chunk_heads, queries, gain_row
        )
        moved.append(from_behind(following, 1))
    second = None
    for c in range(CHUNKS):
        arriving = sent(blocks_of(moved[c], 1, 0))
        local, close = home_calls("home", scalars[1], moved[c], moved_own, near, c, pairs, pairs)
        (second,) = combine_call(
            plan[1], [local, close, *away(arriving, c)], sink_rows[c], second, c, chunk_heads
        )
    return first, second


def solution(mesh):
    both = ("groups", "section")
    rows = P(both, None)
    placed = (rows,) * 5 + (
        P(both, None, None, None),
        P(both, None, None, None),
        rows,
        P(both),
        P(None, both, None),
        P(),
        P(),
    )
    return jax.shard_map(
        body, mesh=mesh, in_specs=placed, out_specs=(rows, rows), check_vma=False
    )
```

```python
import math

import jax
import jax.numpy as jnp
from jax import lax
from jax.experimental import pallas as pl
from jax.experimental.pallas import tpu as pltpu
from jax.sharding import PartitionSpec as P


HEAD = 64
GROUP = 8
QB = 64
REACH = 3
LANES = 128
PAIR = 2 * GROUP * HEAD
KEY_BLOCK = 256
TILE = 1024
ATTEND_VMEM = 32 << 20
COMBINE_VMEM = 16 << 20
CHUNKS = 2
LOG2E = math.log2(math.e)
SCALE2 = LOG2E * HEAD ** -0.5


def from_behind(block, distance, axis="section"):
    size = lax.axis_size(axis)
    route = [((i - distance) % size, i) for i in range(size)]
    return lax.ppermute(block, axis, route)


def stack_heads(q, parity):
    rows = q.shape[0]
    upper = lax.broadcasted_iota(jnp.int32, (rows, LANES), 1) >= HEAD
    keep = upper if parity else jnp.logical_not(upper)
    stacked = []
    for tile in range(GROUP // 2):
        at = parity * GROUP * HEAD + tile * LANES
        both = q[:, at : at + LANES].astype(jnp.float32)
        turned = pltpu.roll(both, HEAD, 1)
        for half in range(2):
            head = both if half == parity else turned
            stacked.append(jnp.where(keep, head, 0.0).astype(jnp.bfloat16))
    return jnp.concatenate(stacked, axis=0)


def attend_pair(q, keys, values, mask_of, out_ref, lane_at, head_at, stats_at, scores, weights):
    rows, used = q.shape[0], keys.shape[0]
    lane = lax.broadcasted_iota(jnp.int32, (rows, LANES), 1)
    peaks = jnp.zeros((rows, LANES), jnp.float32)
    totals = jnp.ones((rows, LANES), jnp.float32)
    with_ones = jnp.concatenate([values, jnp.ones_like(values)], axis=1)
    for parity in range(2):
        stacked = stack_heads(q, parity)
        for start in range(0, used, KEY_BLOCK):
            score = lax.dot_general(
                stacked,
                keys[start : start + KEY_BLOCK],
                (((1,), (1,)), ((), ())),
                preferred_element_type=jnp.float32,
            )
            scores[parity, :, start : start + KEY_BLOCK] = mask_of(score, start)
    for parity in range(2):
        for head in range(GROUP):
            at = head * rows
            peak = jnp.max(scores[parity, at : at + rows, :used], axis=1, keepdims=True)
            peaks = jnp.where(lane == head_at + parity * GROUP + head, peak, peaks)
            for start in range(0, used, KEY_BLOCK):
                score = scores[parity, at : at + rows, start : start + KEY_BLOCK]
                weights[parity, at : at + rows, start : start + KEY_BLOCK] = jnp.exp2(
                    (score - peak) * SCALE2
                ).astype(jnp.bfloat16)
    for parity in range(2):
        both = jnp.dot(
            weights[parity, :, :used], with_ones, preferred_element_type=jnp.float32
        )
        for tile in range(GROUP // 2):
            halves = []
            for half in range(2):
                head = 2 * tile + half
                part = both[head * rows : (head + 1) * rows]
                total = part[:, LANES:]
                part = part[:, :LANES] / total
                halves.append(part if half == parity else pltpu.roll(part, HEAD, 1))
                totals = jnp.where(lane == head_at + parity * GROUP + head, total, totals)
            joined = jnp.where(lane < HEAD, halves[0], halves[1]).astype(jnp.bfloat16)
            start = pl.multiple_of(lane_at + parity * GROUP * HEAD + tile * LANES, LANES)
            out_ref[:, pl.ds(start, LANES)] = joined
    level = peaks * SCALE2 + jnp.log2(totals)
    high = level.astype(jnp.bfloat16).astype(jnp.float32)
    where = pl.ds(pl.multiple_of(stats_at, LANES), LANES)
    stats = out_ref[:, where].astype(jnp.float32)
    stats = stats + high + pltpu.roll(level - high, HEAD, 1)
    out_ref[:, where] = stats.astype(jnp.bfloat16)


def places(pair, pairs, chunk_pairs):
    chunk, inner = lax.div(pair, chunk_pairs), lax.rem(pair, chunk_pairs)
    return pair * PAIR, inner * 2 * GROUP, pairs * PAIR + chunk * LANES


def clear_stats(pair, out_ref, pairs):
    @pl.when(pair == 0)
    def _():
        width = pairs * PAIR
        out_ref[:, width:] = jnp.zeros(
            (out_ref.shape[0], out_ref.shape[1] - width), jnp.bfloat16
        )


def lent_job(length, q, k_ref, v_ref, out_ref, spots, scores, weights):
    lent_rows = k_ref.shape[2]
    half = lent_rows // 2
    for used, now in ((half, length <= half), (lent_rows, length > half)):

        @pl.when(now)
        def _(used=used):
            def mask_of(score, start):
                if used == lent_rows and start < half:
                    return score
                col = lax.broadcasted_iota(jnp.int32, score.shape, 1)
                return jnp.where(col < length - start, score, -jnp.inf)

            attend_pair(
                q,
                k_ref[0, 0, :used, :],
                v_ref[0, 0, :used, :],
                mask_of,
                out_ref,
                *spots,
                scores,
                weights,
            )


def local_job(count, q, ck_ref, cv_ref, sk_ref, sv_ref, out_ref, spots, scores, weights):
    rows, cache_rows = q.shape[0], ck_ref.shape[0]

    def mask_of(score, start):
        row = lax.rem(lax.broadcasted_iota(jnp.int32, score.shape, 0), rows)
        col = lax.broadcasted_iota(jnp.int32, score.shape, 1) + start
        limit = jnp.where(col < cache_rows, count * rows, row + cache_rows + 1)
        return jnp.where(col < limit, score, -jnp.inf)

    attend_pair(
        q,
        jnp.concatenate([ck_ref[...], sk_ref[...]], axis=0),
        jnp.concatenate([cv_ref[...], sv_ref[...]], axis=0),
        mask_of,
        out_ref,
        *spots,
        scores,
        weights,
    )


def local_kernel(index_ref, q_ref, ck, cv, sk, sv, out_ref, scores, weights, *, pairs, chunk_pairs):
    pair = pl.program_id(0)
    clear_stats(pair, out_ref, pairs)
    spots = places(pair, pairs, chunk_pairs)
    local_job(index_ref[0], q_ref[...], ck, cv, sk, sv, out_ref, spots, scores, weights)


def near_kernel(
    len_ref, plan_ref, q_ref, k_ref, v_ref, out_ref, scores, weights, *, pairs, chunk_pairs
):
    pair = pl.program_id(0)
    clear_stats(pair, out_ref, pairs)
    start = pl.multiple_of(plan_ref[0] * QB, QB)
    q = q_ref[pl.ds(start, QB), :]
    spots = places(pair, pairs, chunk_pairs)
    lent_job(len_ref[0], q, k_ref, v_ref, out_ref, spots, scores, weights)


def home_kernel(
    index_ref, len_ref, plan_ref, q_ref, ck, cv, sk, sv, k_ref, v_ref,
    own_ref, near_ref, scores, weights, near_scores, near_weights, *, pairs, chunk_pairs
):
    local_kernel(
        index_ref, q_ref, ck, cv, sk, sv, own_ref, scores, weights,
        pairs=pairs, chunk_pairs=chunk_pairs,
    )
    near_kernel(
        len_ref, plan_ref, q_ref, k_ref, v_ref, near_ref, near_scores, near_weights,
        pairs=pairs, chunk_pairs=chunk_pairs,
    )


def away_kernel(len_ref, *refs, pairs):
    reach = REACH - 1
    q_refs, (k_ref, v_ref) = refs[:reach], refs[reach : reach + 2]
    out_refs, (scores, weights, out) = refs[reach + 2 : 2 * reach + 2], refs[2 * reach + 2 :]
    dist, pair = pl.program_id(0), pl.program_id(1)
    clear_stats(pair, out, pairs)
    q = jnp.where(dist == 0, q_refs[0][...], q_refs[1][...])
    lent_job(
        len_ref[dist + 1], q, k_ref, v_ref, out, places(pair, pairs, pairs), scores, weights
    )
    for d in range(reach):

        @pl.when(jnp.logical_and(dist == d, pair == pairs - 1))
        def _(d=d):
            out_refs[d][...] = out[...]


def scratch(rows, keys):
    return [
        pltpu.VMEM((2, GROUP * rows, keys), jnp.float32),
        pltpu.VMEM((2, GROUP * rows, keys), jnp.bfloat16),
    ]


def estimate(rows, heads, keys):
    return pl.CostEstimate(
        flops=16 * rows * heads * keys * HEAD, bytes_accessed=4 << 20, transcendentals=0
    )


def specs_of(q, cache_keys, near_keys, chunk, pairs):
    rows, base = q.shape[0], chunk * pairs
    q_base = base if q.shape[1] > pairs * PAIR else 0
    q_spec = pl.BlockSpec((rows, PAIR), lambda i, *_: (0, q_base + i))
    cache_spec = pl.BlockSpec((cache_keys.shape[0], LANES), lambda i, *_: (0, base + i))
    own_spec = pl.BlockSpec((rows, LANES), lambda i, *_: (0, base + i))
    near_spec = pl.BlockSpec(
        (1, 1, near_keys.shape[2], LANES), lambda i, *_: (0, 0, 0, base + i)
    )
    return q_spec, [cache_spec, cache_spec, own_spec, own_spec], [near_spec, near_spec]


def packed(rows, pairs, chunk_pairs):
    width = pairs * PAIR + pairs // chunk_pairs * LANES
    return (
        jax.ShapeDtypeStruct((rows, width), jnp.bfloat16),
        pl.BlockSpec((rows, width), lambda i, *_: (0, 0)),
    )


def home_calls(parts, scalars, q, own, near, chunk, pairs, chunk_pairs):
    index, lengths, plan = scalars
    rows = q.shape[0]
    q_spec, own_specs, near_specs = specs_of(q, own[0], near[0], chunk, pairs)
    own_out, own_out_spec = packed(rows, pairs, chunk_pairs)
    near_out, near_out_spec = packed(QB, pairs, chunk_pairs)
    keys = own[0].shape[0] + own[2].shape[0]
    lent_rows = near[0].shape[2]
    kernel, ins, specs, outs, out_specs, buffers, cost = {
        "local": (
            local_kernel, (index, q, *own), own_specs, own_out, own_out_spec,
            scratch(rows, keys), estimate(rows, 16 * pairs, keys),
        ),
        "near": (
            near_kernel, (lengths, plan, q, *near), near_specs, near_out, near_out_spec,
            scratch(QB, lent_rows), estimate(QB, 16 * pairs, lent_rows),
        ),
        "home": (
            home_kernel, (index, lengths, plan, q, *own, *near), own_specs + near_specs,
            [own_out, near_out], [own_out_spec, near_out_spec],
            scratch(rows, keys) + scratch(QB, lent_rows),
            estimate(rows, 32 * pairs, keys),
        ),
    }[parts]
    return pl.pallas_call(
        lambda *refs: kernel(*refs, pairs=pairs, chunk_pairs=chunk_pairs),
        grid_spec=pltpu.PrefetchScalarGridSpec(
            num_scalar_prefetch=len(ins) - len(specs) - 1,
            grid=(pairs,),
            in_specs=[q_spec] + specs,
            out_specs=out_specs,
            scratch_shapes=buffers,
        ),
        out_shape=outs,
        cost_estimate=cost,
        compiler_params=pltpu.CompilerParams(vmem_limit_bytes=ATTEND_VMEM),
    )(*ins)


def away_call(lengths, blocks, keys, values, chunk, pairs):
    reach = REACH - 1
    lent_rows = keys.shape[2]
    width = pairs * PAIR + LANES
    kv_spec = pl.BlockSpec(
        (1, 1, lent_rows, LANES), lambda d, i, *_: (0, d + 1, 0, chunk * pairs + i)
    )
    return pl.pallas_call(
        lambda *refs: away_kernel(*refs, pairs=pairs),
        grid_spec=pltpu.PrefetchScalarGridSpec(
            num_scalar_prefetch=1,
            grid=(reach, pairs),
            in_specs=[
                pl.BlockSpec((QB, PAIR), lambda d, i, *_: (0, jnp.where(d == 0, i, pairs - 1))),
                pl.BlockSpec((QB, PAIR), lambda d, i, *_: (0, jnp.where(d == 0, 0, i))),
                kv_spec,
                kv_spec,
            ],
            out_specs=[pl.BlockSpec((QB, width), lambda d, i, *_: (0, 0))] * reach,
            scratch_shapes=scratch(QB, lent_rows) + [pltpu.VMEM((QB, width), jnp.bfloat16)],
        ),
        out_shape=[jax.ShapeDtypeStruct((QB, width), jnp.bfloat16)] * reach,
        cost_estimate=estimate(QB, 32 * pairs, lent_rows),
        compiler_params=pltpu.CompilerParams(vmem_limit_bytes=ATTEND_VMEM),
        name="away",
    )(lengths, *blocks, keys, values)


def two_parts(x):
    high = x.astype(jnp.bfloat16)
    low = (x - high.astype(jnp.float32)).astype(jnp.bfloat16)
    return jnp.concatenate([high, low], axis=1)


def picks(count, first, parts=2):
    shape = (parts * count, TILE)
    head = lax.div(lax.broadcasted_iota(jnp.int32, shape, 1), HEAD) + first
    row = lax.rem(lax.broadcasted_iota(jnp.int32, shape, 0), count)
    return jnp.where(head == row, 1.0, 0.0).astype(jnp.bfloat16)


def combine_kernel(plan_ref, *refs, heads, form_next, aliased):
    groups = REACH + 1
    data, stats = refs[:groups], refs[groups : 2 * groups]
    sink_ref, rest = refs[2 * groups], refs[2 * groups + 1 :]
    if form_next:
        q_ref, gain_ref = rest[:2]
        rest = rest[2:]
    rest = rest[aliased:]
    out_ref = rest[0]
    acc, levels, parts = rest[-3:]
    rows = data[0].shape[0]
    step = pl.program_id(0)
    starts = [pl.multiple_of(plan_ref[d] * QB, QB) for d in range(REACH)]

    @pl.when(step == 0)
    def _():
        def level_of(ref):
            both = ref[...].astype(jnp.float32)
            return both[:, :heads] + both[:, HEAD : HEAD + heads]

        sink = sink_ref[...] * LOG2E
        levels[1:] = jnp.full((REACH, rows, heads), -jnp.inf, jnp.float32)
        levels[0] = level_of(stats[0])
        for d in range(REACH):
            levels[d + 1, pl.ds(starts[d], QB), :] = level_of(stats[d + 1])
        top = jnp.maximum(levels[0], sink)
        for d in range(REACH):
            top = jnp.maximum(top, levels[d + 1])
        denom = jnp.exp2(sink - top)
        for g in range(groups):
            weight = jnp.exp2(levels[g] - top)
            denom = denom + weight
            levels[g] = weight
        share = 1.0 / denom
        parts[:rows, :] = two_parts(levels[0] * share)
        levels[0] = share
        for d in range(REACH):
            at = pl.ds(starts[d], QB)
            parts[rows + d * QB : rows + (d + 1) * QB, :] = two_parts(
                levels[d + 1, at, :] * levels[0, at, :]
            )

    spread = jnp.dot(
        parts[...], picks(heads, step * (TILE // HEAD)), preferred_element_type=jnp.float32
    )
    acc[...] = data[0][...].astype(jnp.float32) * spread[:rows]
    for d in range(REACH):
        at = pl.ds(starts[d], QB)
        share = spread[rows + d * QB : rows + (d + 1) * QB]
        acc[at, :] = acc[at, :] + data[d + 1][...].astype(jnp.float32) * share
    out = acc[...].astype(jnp.bfloat16)
    out_ref[...] = out
    if form_next:
        stream = q_ref[...].astype(jnp.float32) + out.astype(jnp.float32)
        count = LANES // 2
        pick = picks(count, 0)
        high_low = two_parts(stream * stream)
        pick_sum = picks(LANES, 0, 1)
        contract = (((1,), (1,)), ((), ()))
        sums = lax.dot_general(
            high_low[:, :TILE], pick_sum, contract, preferred_element_type=jnp.float32
        ) + lax.dot_general(
            high_low[:, TILE:], pick_sum, contract, preferred_element_type=jnp.float32
        )
        inverse = lax.rsqrt(sums[:, :count] * (1.0 / HEAD) + 1e-06)
        factor = jnp.dot(two_parts(inverse), pick, preferred_element_type=jnp.float32)
        rest[1][...] = (stream * factor * gain_ref[...]).astype(jnp.bfloat16)


def combine_call(plan, groups, sinks, before, chunk, chunk_heads, queries=None, gain=None):
    rows = groups[0].shape[0]
    width = chunk_heads * HEAD
    tiles = width // TILE
    whole_width = CHUNKS * width
    form_next = queries is not None
    data_specs, stats_specs = [], []
    for group in groups:
        wide = group.shape[1] > width + LANES
        base = chunk * tiles if wide else 0
        stat = whole_width // LANES + chunk if wide else width // LANES
        data_specs.append(
            pl.BlockSpec((group.shape[0], TILE), lambda i, *_, base=base: (0, base + i))
        )
        stats_specs.append(
            pl.BlockSpec((group.shape[0], LANES), lambda i, *_, stat=stat: (0, stat))
        )
    ins = [plan, *groups, *groups, sinks]
    specs = data_specs + stats_specs + [pl.BlockSpec((1, chunk_heads), lambda i, *_: (0, 0))]
    place = pl.BlockSpec((rows, TILE), lambda i, *_: (0, chunk * tiles + i))
    outs = [jax.ShapeDtypeStruct((rows, whole_width), jnp.bfloat16)]
    out_specs = [place]
    if form_next:
        ins += [queries, gain]
        specs += [place, pl.BlockSpec((1, TILE), lambda i, *_: (0, chunk * tiles + i))]
        outs.append(jax.ShapeDtypeStruct((rows, width), jnp.bfloat16))
        out_specs.append(pl.BlockSpec((rows, TILE), lambda i, *_: (0, i)))
    aliases = {}
    if before is not None:
        aliases = {len(ins): 0}
        ins.append(before)
        specs.append(pl.BlockSpec(memory_space=pl.ANY))
    return pl.pallas_call(
        lambda *refs: combine_kernel(
            *refs, heads=chunk_heads, form_next=form_next, aliased=len(aliases)
        ),
        grid_spec=pltpu.PrefetchScalarGridSpec(
            num_scalar_prefetch=1,
            grid=(tiles,),
            in_specs=specs,
            out_specs=out_specs,
            scratch_shapes=[
                pltpu.VMEM((rows, TILE), jnp.float32),
                pltpu.VMEM((REACH + 1, rows, chunk_heads), jnp.float32),
                pltpu.VMEM((rows + REACH * QB, 2 * chunk_heads), jnp.bfloat16),
            ],
        ),
        out_shape=outs,
        input_output_aliases=aliases,
        cost_estimate=pl.CostEstimate(
            flops=1 << 29, bytes_accessed=4 << 20, transcendentals=0
        ),
        compiler_params=pltpu.CompilerParams(vmem_limit_bytes=COMBINE_VMEM),
        name="combine",
    )(*ins)


def body(
    queries,
    slice_keys,
    slice_values,
    cache_keys,
    cache_values,
    lent_keys,
    lent_values,
    lent_len,
    slice_index,
    lend_block,
    sinks,
    gain,
):
    heads = queries.shape[1] // HEAD
    chunk_heads = heads // CHUNKS
    width = chunk_heads * HEAD
    all_pairs = heads // (2 * GROUP)
    pairs = all_pairs // CHUNKS
    plan = lend_block[:, 0, :]
    lengths = lent_len[0]
    gain_row = gain[None, :]
    sink_rows = [sinks[c * chunk_heads : (c + 1) * chunk_heads][None, :] for c in range(CHUNKS)]

    def blocks_of(current, step, lane):
        return [
            lax.dynamic_slice(current, (plan[step, d] * QB, jnp.int32(lane)), (QB, width))
            for d in range(1, REACH)
        ]

    def sent(blocks):
        return [from_behind(block, d + 2) for d, block in enumerate(blocks)]

    def returned(parts):
        return [from_behind(part, -(d + 2)) for d, part in enumerate(parts)]

    def away(arrived, chunk):
        parts = away_call(lengths, arrived, lent_keys, lent_values, chunk, pairs)
        return returned(parts)

    arrived = [sent(blocks_of(queries, 0, c * width)) for c in range(CHUNKS)]
    near = (from_behind(lent_keys[:, :1], -1), from_behind(lent_values[:, :1], -1))
    near_lengths = from_behind(lengths, -1)
    moved_own = (cache_keys, cache_values, from_behind(slice_keys, 1), from_behind(slice_values, 1))
    own = (cache_keys, cache_values, slice_keys, slice_values)
    scalars = [(slice_index, near_lengths, plan[step]) for step in range(2)]
    local = home_calls("local", scalars[0], queries, own, near, 0, all_pairs, pairs)
    far = [away(arrived[c], c) for c in range(CHUNKS)]
    close = home_calls("near", scalars[0], queries, own, near, 0, all_pairs, pairs)
    first, moved = None, []
    for c in range(CHUNKS):
        first, following = combine_call(
            plan[0], [local, close, *far[c]], sink_rows[c], first, c, chunk_heads,
            queries, gain_row,
        )
        moved.append(from_behind(following, 1))
    second = None
    for c in range(CHUNKS):
        arriving = sent(blocks_of(moved[c], 1, 0))
        local, close = home_calls("home", scalars[1], moved[c], moved_own, near, c, pairs, pairs)
        parts = away(arriving, c)
        (second,) = combine_call(
            plan[1], [local, close, *parts], sink_rows[c], second, c, chunk_heads
        )
    return first, second


def solution(mesh):
    both = ("groups", "section")
    rows = P(both, None)
    placed = (rows,) * 5 + (
        P(both, None, None, None),
        P(both, None, None, None),
        rows,
        P(both),
        P(None, both, None),
        P(),
        P(),
    )

    return jax.shard_map(body, mesh=mesh, in_specs=placed, out_specs=(rows, rows), check_vma=False)
```
